256 devices in a mesh: depth: 16 (over z, core), gx: 16 (over y, x).
Axes of the slice: x: 4, y: 4, z: 8, core: 2. Of those that a mesh axis runs over, the one named last changes fastest.
Arguments:
- pressure_now: float32 [4, 512, 512, 128], P(None, 'gx', 'depth'), may hold values from -6 to 6
- pressure_before: float32 [4, 512, 512, 128], P(None, 'gx', 'depth'), may hold values from -6 to 6
- class_map: int32 [512, 512, 128], P('gx', 'depth'), may hold values from 0 to 7
- courant_sq: float32 [8], replicated, may hold values from 0.02 to 0.12
- source_cells: int32 [4, 3], replicated, may hold values from 0 to 511, as said below
- source_wavelet: float32 [8, 4], replicated, may hold values from -6 to 6
- layer_start: int32 [1], replicated, may hold values from 488 to 496
Outputs:
- pressure_final: float32 [4, 512, 512, 128], P(None, 'gx', 'depth')
- pressure_prior: float32 [4, 512, 512, 128], P(None, 'gx', 'depth')
The draws below stay inside these ranges and needn't reach their ends.
Inputs may be any that keep to these rules, and one draw needn't show every extreme that they name: `source_cells`: each row holds a cell inside the grid: x below 512, depth below 512, y below 128; shot 0 sits at the last cell along every dimension and shot 1 at cell (0, 0, 0).
All inputs are finite; a program needn't handle non-finite values.
Results may differ from the reference program's by a relative error of at most 0.00002.
Values sent between devices are 32-bit elements; how exact they have to be, the bound alone decides.
No kernel may reach another device: no remote copies, remote signals or barrier semaphores. Data moves between devices by JAX's collectives and lax.ppermute only.
A program may use at most 128 MiB of HBM per device.

```python
import math
import jax
import jax.numpy as jnp

NY = 128
SHOTS = 4
ITERS = 8
CLASSES = 8
NX = 512
NZ = 512


def draw_source_cells(key, part):
    key_x = jax.random.fold_in(key, 11)
    key_z = jax.random.fold_in(key, 12)
    key_y = jax.random.fold_in(key, 13)
    cell_x = jax.random.randint(key_x, (SHOTS,), 0, NX, dtype=jnp.int32)
    cell_z = jax.random.randint(key_z, (SHOTS,), 0, NZ, dtype=jnp.int32)
    cell_y = jax.random.randint(key_y, (SHOTS,), 0, NY, dtype=jnp.int32)
    cell_x = cell_x.at[0].set(jnp.int32(NX - 1)).at[1].set(jnp.int32(0))
    cell_z = cell_z.at[0].set(jnp.int32(NZ - 1)).at[1].set(jnp.int32(0))
    cell_y = cell_y.at[0].set(jnp.int32(NY - 1)).at[1].set(jnp.int32(0))
    return jnp.stack([cell_x, cell_z, cell_y], axis=1)


def plant(entries, own_key, low, top_value):
    longest = entries.shape.index(max(entries.shape))
    spots = []
    for shift in (0, 1):
        where = [jax.random.randint(jax.random.fold_in(own_key, axis), (), 0, length) for axis, length in enumerate(entries.shape)]
        where[longest] = (where[longest] + shift) % entries.shape[longest]
        spots.append(tuple(where))
    return entries.at[spots[0]].set(low).at[spots[1]].set(top_value)


def block_scale(key, dims, shards, smallest, top_value):
    def one(axis_at, blocks):
        draws = jax.random.uniform(jax.random.fold_in(jax.random.fold_in(key, 6), axis_at), (blocks,), jnp.float32, smallest / len(shards), top_value / len(shards))
        return jnp.repeat(jnp.exp(draws), dims[axis_at] // blocks).reshape((-1,) + (1,) * (len(dims) - axis_at - 1))

    gain = one(*shards[0])
    for cut in shards[1:]:
        gain = gain * one(*cut)
    return gain


def noise(stream_key, dims, spread, bound, cuts=(), kind=jnp.bfloat16):
    drawn = jax.random.normal(stream_key, dims, jnp.float32) * spread
    if len(cuts) > 0:
        drawn = block_scale(stream_key, dims, cuts, -0.22, 0.18) * drawn
    return jnp.clip(drawn, min=-bound, max=bound).astype(kind)


def setup_inputs(seed: int = 0) -> dict:
    key_of = jax.random.split(jax.random.key(seed), 8)
    pressure_now = noise(key_of[0], (SHOTS, NX, NZ, NY), 1.0, 6.0, ((1, 16), (2, 16)), jnp.float32)
    pressure_before = noise(key_of[1], (SHOTS, NX, NZ, NY), 1.0, 6.0, ((1, 16), (2, 16)), jnp.float32)
    class_map = plant(jax.random.randint(key_of[2], (NX, NZ, NY), 0, CLASSES), jax.random.fold_in(key_of[2], 1), 0, CLASSES - 1).astype(jnp.int32)
    courant_sq = jnp.clip(jnp.exp(jax.random.uniform(key_of[3], (CLASSES,), jnp.float32, math.log(0.02), math.log(0.12))), 0.02, 0.12)
    source_cells = draw_source_cells(jax.random.fold_in(key_of[7], 71), 0)
    source_wavelet = noise(key_of[5], (ITERS, SHOTS), 1.0, 6.0, (), jnp.float32)
    layer_start = jax.random.randint(key_of[6], (1,), NZ - 24, NZ - 15).astype(jnp.int32)
    return dict(pressure_now=pressure_now, pressure_before=pressure_before, class_map=class_map, courant_sq=courant_sq, source_cells=source_cells, source_wavelet=source_wavelet, layer_start=layer_start)


COEFFS = (-205.0 / 72.0, 8.0 / 5.0, -1.0 / 5.0, 8.0 / 315.0, -1.0 / 560.0)
DAMPING = 0.3


def laplace(padded, rows, depth):
    center = padded[:, 4:4 + rows, 4:4 + depth, :]
    total = 3.0 * COEFFS[0] * center
    side_y = jnp.pad(center, ((0, 0), (0, 0), (0, 0), (4, 4)))
    width = center.shape[3]
    for k in range(1, 5):
        pair = padded[:, 4 + k:4 + k + rows, 4:4 + depth, :] + padded[:, 4 - k:4 - k + rows, 4:4 + depth, :]
        pair = pair + padded[:, 4:4 + rows, 4 + k:4 + k + depth, :] + padded[:, 4:4 + rows, 4 - k:4 - k + depth, :]
        pair = pair + side_y[:, :, :, 4 + k:4 + k + width] + side_y[:, :, :, 4 - k:4 - k + width]
        total = total + COEFFS[k] * pair
    return total


def advance(current, before, padded, speed, damping, source):
    lap = laplace(padded, current.shape[1], current.shape[2])
    return (2.0 * current - (1.0 - damping) * before + speed * lap + source) / (1.0 + damping)


def profile(global_z, start, total):
    ratio = (global_z - start + 1).astype(jnp.float32) / (total - start).astype(jnp.float32)
    return jnp.where(global_z >= start, DAMPING * ratio * ratio, jnp.float32(0.0))


def point_mask(cells, column, anchor, count):
    index = anchor + jnp.arange(count, dtype=jnp.int32)
    return (index[None, :] == cells[:, column][:, None]).astype(jnp.float32)


def reference(pressure_now, pressure_before, class_map, courant_sq, source_cells, source_wavelet, layer_start):
    speed = courant_sq[class_map]
    depth_index = jnp.arange(NZ, dtype=jnp.int32)
    damping = profile(depth_index, layer_start[0], jnp.int32(NZ))[None, None, :, None]
    mask_x = point_mask(source_cells, 0, jnp.int32(0), NX)
    mask_z = point_mask(source_cells, 1, jnp.int32(0), NZ)
    mask_y = point_mask(source_cells, 2, jnp.int32(0), NY)
    onehot = mask_x[:, :, None, None] * mask_z[:, None, :, None] * mask_y[:, None, None, :]
    current, before = pressure_now, pressure_before
    for step in range(ITERS):
        padded = jnp.pad(current, ((0, 0), (4, 4), (4, 4), (0, 0)))
        source = source_wavelet[step][:, None, None, None] * onehot
        nxt = advance(current, before, padded, speed, damping, source)
        before, current = current, nxt
    return current, before
```

```python
import jax
import jax.numpy as jnp
from jax import lax
from jax.sharding import PartitionSpec as P

ITERS = 8


COEFFS = (-205.0 / 72.0, 8.0 / 5.0, -1.0 / 5.0, 8.0 / 315.0, -1.0 / 560.0)
DAMPING = 0.3


def padded_2(shard, sides, width):
    edges = {}
    for axis, dim in sides:
        peers, length = (lax.axis_size(axis), shard.shape[dim])
        up = [(i, (i + 1) % peers) for i in range(peers)]
        last = lax.slice_in_dim(shard, length - width, length, axis=dim)
        leading = lax.slice_in_dim(shard, 0, width, axis=dim)
        place = lax.axis_index(axis)
        low = lax.ppermute(last, axis, up)
        high = lax.ppermute(leading, axis, [(b, a) for a, b in up])
        edges[dim] = (
            jnp.where(place > 0, low, 0.0),
            jnp.where(place < peers - 1, high, 0.0),
        )
    done = []
    for _, dim in sides:
        low, high = edges[dim]
        around = [(width, width) if d in done else (0, 0) for d in range(shard.ndim)]
        shard = jnp.concatenate([jnp.pad(low, around), shard, jnp.pad(high, around)], axis=dim)
        done.append(dim)
    return shard


def laplace(padded, rows, depth):
    center = padded[:, 4 : 4 + rows, 4 : 4 + depth, :]
    total = 3.0 * COEFFS[0] * center
    side_y = jnp.pad(center, ((0, 0), (0, 0), (0, 0), (4, 4)))
    width = center.shape[3]
    for k in range(1, 5):
        pair = (
            padded[:, 4 + k : 4 + k + rows, 4 : 4 + depth, :]
            + padded[:, 4 - k : 4 - k + rows, 4 : 4 + depth, :]
        )
        pair = (
            pair
            + padded[:, 4 : 4 + rows, 4 + k : 4 + k + depth, :]
            + padded[:, 4 : 4 + rows, 4 - k : 4 - k + depth, :]
        )
        pair = (
            pair + side_y[:, :, :, 4 + k : 4 + k + width] + side_y[:, :, :, 4 - k : 4 - k + width]
        )
        total = total + COEFFS[k] * pair
    return total


def advance(current, before, padded, speed, damping, source):
    lap = laplace(padded, current.shape[1], current.shape[2])
    return (2.0 * current - (1.0 - damping) * before + speed * lap + source) / (1.0 + damping)


def profile(global_z, start, total):
    ratio = (global_z - start + 1).astype(jnp.float32) / (total - start).astype(jnp.float32)
    return jnp.where(global_z >= start, DAMPING * ratio * ratio, jnp.float32(0.0))


def point_mask(cells, column, anchor, count):
    index = anchor + jnp.arange(count, dtype=jnp.int32)
    return (index[None, :] == cells[:, column][:, None]).astype(jnp.float32)


def lookup_speed(class_map, courant_sq):
    speed = jnp.zeros(class_map.shape, jnp.float32)
    for klass in range(courant_sq.shape[0]):
        speed = speed + jnp.where(class_map == klass, courant_sq[klass], jnp.float32(0.0))
    return speed


def local(
    pressure_now, pressure_before, class_map, courant_sq, source_cells, source_wavelet, layer_start
):
    rows = pressure_now.shape[1]
    depth = pressure_now.shape[2]
    width = pressure_now.shape[3]
    x_anchor = lax.axis_index("gx") * rows
    z_anchor = lax.axis_index("depth") * depth
    total_z = jnp.int32(depth * lax.axis_size("depth"))
    speed = lookup_speed(class_map, courant_sq)
    mask_y = point_mask(source_cells, 2, jnp.int32(0), width)
    current, before = (pressure_now, pressure_before)
    mask_x = point_mask(source_cells, 0, x_anchor, rows)
    depth_index = z_anchor + jnp.arange(depth, dtype=jnp.int32)
    damping = profile(depth_index, layer_start[0], total_z)[None, None, :, None]
    mask_z = point_mask(source_cells, 1, z_anchor, depth)
    onehot = mask_x[:, :, None, None] * mask_z[:, None, :, None] * mask_y[:, None, None, :]
    for step in range(ITERS):
        padded = padded_2(current, (("gx", 1), ("depth", 2)), 4)
        source = source_wavelet[step][:, None, None, None] * onehot
        nxt = advance(current, before, padded, speed, damping, source)
        before, current = (current, nxt)
    return (current, before)


def solution(mesh):
    placed = (
        P(None, "gx", "depth", None),
        P(None, "gx", "depth", None),
        P("gx", "depth", None),
        P(),
        P(),
        P(),
        P(),
    )
    return jax.shard_map(
        local,
        mesh=mesh,
        in_specs=placed,
        out_specs=(P(None, "gx", "depth", None), P(None, "gx", "depth", None)),
        check_vma=False,
    )
```

```python
import jax
import jax.numpy as jnp
from jax import lax
from jax.experimental import pallas as pl
from jax.experimental.pallas import tpu as pltpu
from jax.sharding import PartitionSpec as P


ITERS = 8
COEFFS = (-205.0 / 72.0, 8.0 / 5.0, -1.0 / 5.0, 8.0 / 315.0, -1.0 / 560.0)
DAMPING = 0.3
HALO = 4
ZO = 8
F32 = jnp.float32


def lanes(rows, width):
    return lax.broadcasted_iota(jnp.int32, (rows, width), 1)


def stencil(u, v, w, sa, bc, s, x, z, count):
    width = u.shape[3]
    at = ZO + z
    center = u[s, HALO + x, at : at + count, :]
    lane = lanes(count, width)
    total = None
    for k in range(1, HALO + 1):
        pair = u[s, HALO + x + k, at : at + count, :] + u[s, HALO + x - k, at : at + count, :]
        pair = pair + (u[s, HALO + x, at + k : at + k + count, :] + u[s, HALO + x, at - k : at - k + count, :])
        low = jnp.where(lane >= k, pltpu.roll(center, k, 1), 0.0)
        high = jnp.where(lane < width - k, pltpu.roll(center, width - k, 1), 0.0)
        pair = pair + (low + high)
        total = COEFFS[k] * pair if total is None else total + COEFFS[k] * pair
    return (
        w[x, z : z + count, :] * center
        + sa[x, z : z + count, :] * total
        - bc[z : z + count, :] * v[s, HALO + x, at : at + count, :]
    )


def inject(step, spot, amp, v, spans, send=None, send_at=None):
    shots, width = v.shape[0], v.shape[3]
    depth = v.shape[2] - 2 * ZO

    @pl.when(spot[shots : shots + 1, :][0, 0] >= 0)
    def _():
        for s in range(shots):
            flat = spot[s : s + 1, :][0, 0]
            x = lax.div(flat, depth * width)
            z = lax.rem(lax.div(flat, width), depth)
            y = lax.rem(flat, width)
            for x_low, x_high, z_low, z_high in spans:

                @pl.when((flat >= 0) & (x >= x_low) & (x < x_high) & (z >= z_low) & (z < z_high))
                def _():
                    at = step * shots + s
                    add = jnp.where(lanes(1, width) == y, amp[at : at + 1, :], 0.0)
                    row = v[s, HALO + x, pl.ds(ZO + z, 1), :] + add
                    v[s, HALO + x, pl.ds(ZO + z, 1), :] = row
                    if send is not None:
                        send[s, x - send_at, pl.ds(z, 1), :] = row


def at_high_x(side):
    odd = lax.rem(lax.axis_index("gx"), 2)
    return odd if side == 0 else 1 - odd


def at_end(axis):
    place = lax.axis_index(axis)
    return (place == 0) | (place == lax.axis_size(axis) - 1)


def fill_depth(u, z_near, z_far, columns, depth):
    odd = lax.rem(lax.axis_index("depth"), 2) == 1
    inside = jnp.where(at_end("depth"), 0.0, 1.0).astype(F32)

    def some(x, carry):
        for s in range(u.shape[0]):
            far = z_far[s, x]
            near = z_near[s, x] * inside
            u[s, HALO + x, ZO - HALO : ZO, :] = jnp.where(odd, far, near)
            u[s, HALO + x, ZO + depth : ZO + depth + HALO, :] = jnp.where(odd, near, far)
        return carry

    lax.fori_loop(0, columns, some, 0, unroll=8)


def fill_x(side, u, got, columns, depth):
    at = at_high_x(side) * (columns + HALO)
    inside = jnp.where(at_end("gx"), 0.0, 1.0).astype(F32)
    for s in range(u.shape[0]):
        for x in range(HALO):
            row = got[s, x]
            u[s, at + x, ZO : ZO + depth, :] = row * inside if side == 0 else row


def depth_faces(v, send_near, send_far, columns, depth):
    odd = lax.rem(lax.axis_index("depth"), 2) == 1

    def face(x, carry):
        for s in range(v.shape[0]):
            low = v[s, HALO + x, ZO : ZO + HALO, :]
            high = v[s, HALO + x, ZO + depth - HALO : ZO + depth, :]
            send_near[s, x] = jnp.where(odd, high, low)
            send_far[s, x] = jnp.where(odd, low, high)
        return carry

    lax.fori_loop(0, columns, face, 0, unroll=8)


def span_loop(u, v, w, sa, bc, tiles, group):
    inner = w.shape[0] - 2 * HALO

    def some(i, carry):
        s, x = i // (inner // group), HALO + group * lax.rem(i, inner // group)
        for j in range(group):
            for z, count in tiles:
                v[s, HALO + x + j, ZO + z : ZO + z + count, :] = stencil(u, v, w, sa, bc, s, x + j, z, count)
        return carry

    lax.fori_loop(0, v.shape[0] * (inner // group), some, 0)


def ends_kernel(step, spot, amp, u_in, v_in, z_near, z_far, w, sa, bc, u, v, *out):
    del u_in, v_in
    columns, depth = w.shape[0], w.shape[1]
    fill_depth(u, z_near, z_far, columns, depth)
    span_loop(u, v, w, sa, bc, ((0, 8), (depth - 8, 8)), 12)
    inject(step, spot, amp, v, ((HALO, columns - HALO, 0, 8), (HALO, columns - HALO, depth - 8, depth)))
    if step == ITERS - 1:
        to_hbm(v, *out, ((HALO, columns - 2 * HALO),))


def middle_kernel(step, spot, amp, u, v_in, w, sa, bc, v):
    del v_in
    columns, depth = w.shape[0], w.shape[1]
    span_loop(u, v, w, sa, bc, ((8, depth - 16),), 12)
    inject(step, spot, amp, v, ((HALO, columns - HALO, 8, depth - 8),))


def edge_kernel(step, spot, amp, u_in, v_in, got_b, got_a, w, sa, bc, u, v, near, far, send_b, send_a):
    del u_in, v_in
    columns, depth = w.shape[0], w.shape[1]
    fill_x(0, u, got_b, columns, depth)
    fill_x(1, u, got_a, columns, depth)
    for s in range(u.shape[0]):
        for x in range(HALO):
            for side, send in ((0, send_b), (1, send_a)):
                at = at_high_x(side) * (columns - HALO) + x
                new = stencil(u, v, w, sa, bc, s, at, 0, depth)
                v[s, HALO + at, ZO : ZO + depth, :] = new
                send[s, x] = new
    for side, send in ((0, send_b), (1, send_a)):
        face = at_high_x(side) * (columns - HALO)
        inject(step, spot, amp, v, ((face, face + HALO, 0, depth),), send, face)
    depth_faces(v, near, far, columns, depth)


def last_kernel(step, spot, amp, u_in, v_in, out_in, got_b, got_a, w, sa, bc, u, v, out, sem):
    del u_in, v_in, out_in
    columns, depth = w.shape[0], w.shape[1]
    fill_x(0, u, got_b, columns, depth)
    fill_x(1, u, got_a, columns, depth)
    for s in range(u.shape[0]):
        for x in range(HALO):
            for at in (x, columns - HALO + x):
                v[s, HALO + at, ZO : ZO + depth, :] = stencil(u, v, w, sa, bc, s, at, 0, depth)
    inject(step, spot, amp, v, ((0, HALO, 0, depth), (columns - HALO, columns, 0, depth)))
    to_hbm(v, out, sem, ((0, HALO), (columns - HALO, HALO)))


def to_hbm(v, out, sem, spans):
    shots, depth = out.shape[0], out.shape[2]
    copies = []
    for i, (first, count) in enumerate(spans):
        for s in range(shots):
            source = v.at[s, pl.ds(HALO + first, count), pl.ds(ZO, depth), :]
            copies.append(pltpu.make_async_copy(source, out.at[s, pl.ds(first, count)], sem.at[i * shots + s]))
    for c in copies:
        c.start()
    for c in copies:
        c.wait()


def prior_kernel(u, out, sem):
    to_hbm(u, out, sem, ((0, out.shape[1]),))


def open_kernel(now, send_b, send_a, send_near, send_far, low, high, sem):
    shots, columns, depth = now.shape[0], now.shape[1], now.shape[2]
    copies = []
    for target, source in (
        (low, now.at[:, :, pl.ds(0, 8)]),
        (high, now.at[:, :, pl.ds(depth - 8, 8)]),
        (send_b, now.at[:, pl.ds(at_high_x(0) * (columns - HALO), HALO)]),
        (send_a, now.at[:, pl.ds(at_high_x(1) * (columns - HALO), HALO)]),
    ):
        copies.append(pltpu.make_async_copy(source, target, sem.at[len(copies)]))
    for c in copies:
        c.start()
    odd = lax.rem(lax.axis_index("depth"), 2) == 1
    copies[0].wait()
    copies[1].wait()

    def face(x, carry):
        for s in range(shots):
            first, last = low[s, x, 0:HALO, :], high[s, x, 8 - HALO : 8, :]
            send_near[s, x] = jnp.where(odd, last, first)
            send_far[s, x] = jnp.where(odd, first, last)
        return carry

    lax.fori_loop(0, columns, face, 0, unroll=8)
    copies[2].wait()
    copies[3].wait()


def begin_kernel(speeds, start, cells, wavelet, now, before, classes, u, v, w, sa, bc, spot, amp, kinds, sem):
    shots, columns, depth, width = now.shape
    copies = [pltpu.make_async_copy(classes, kinds, sem.at[2 * shots])]
    for i, (source, state) in enumerate(((now, u), (before, v))):
        for s in range(shots):
            target = state.at[s, pl.ds(HALO, columns), pl.ds(ZO, depth), :]
            copies.append(pltpu.make_async_copy(source.at[s], target, sem.at[i * shots + s]))
    for c in copies:
        c.start()
    total = depth * lax.axis_size("depth")
    first_x, first_z = lax.axis_index("gx") * columns, lax.axis_index("depth") * depth
    begin = start[0]

    def damping_at(z):
        ratio = (z - begin + 1).astype(F32) / jnp.broadcast_to((total - begin).astype(F32), z.shape)
        return jnp.where(z >= begin, DAMPING * ratio * ratio, 0.0)

    damping = damping_at(first_z + lax.broadcasted_iota(jnp.int32, (depth, width), 0))
    inverse = 1.0 / (1.0 + damping)
    bc[...] = (1.0 - damping) * inverse
    some = jnp.int32(-1)
    for s in range(shots):
        x, z, y = cells[s, 0] - first_x, cells[s, 1] - first_z, cells[s, 2]
        mine = (x >= 0) & (x < columns) & (z >= 0) & (z < depth)
        flat = jnp.where(mine, (x * depth + z) * width + y, -1)
        some = jnp.maximum(some, flat)
        spot[s : s + 1, :] = jnp.broadcast_to(flat, (1, width))
        scale = 1.0 / (1.0 + damping_at(jnp.broadcast_to(cells[s, 1], (1, width))))
        for step in range(wavelet.shape[0]):
            amp[step * shots + s : step * shots + s + 1, :] = wavelet[step, s] * scale
    spot[shots : shots + 1, :] = jnp.broadcast_to(some, (1, width))
    copies[0].wait()

    def column(x, carry):
        kind = kinds[x]
        speed = jnp.zeros((depth, width), F32)
        for c in range(speeds.shape[0]):
            speed = jnp.where(kind == c, speeds[c], speed)
        scaled = speed * inverse
        sa[x] = scaled
        w[x] = 2.0 * inverse + (3.0 * COEFFS[0]) * scaled
        return carry

    lax.fori_loop(0, columns, column, 0, unroll=2)
    for c in copies[1:]:
        c.wait()


VMEM = pl.BlockSpec(memory_space=pltpu.VMEM)
SMEM = pl.BlockSpec(memory_space=pltpu.SMEM)
ANY = pl.BlockSpec(memory_space=pl.ANY)


def call(kernel, out_shape, args, specs, aliases=None, flops=1_000_000, scratch=(), out_specs=None):
    return pl.pallas_call(
        kernel,
        out_shape=out_shape,
        in_specs=specs,
        out_specs=out_specs if out_specs is not None else [VMEM] * len(out_shape),
        input_output_aliases=aliases or {},
        scratch_shapes=list(scratch),
        cost_estimate=pl.CostEstimate(flops=flops, bytes_accessed=4_000_000, transcendentals=0),
        compiler_params=pltpu.CompilerParams(vmem_limit_bytes=16 * 1024 * 1024),
    )(*args)


def pairs(count):
    b = [(i, (i - 1) % count if i % 2 == 0 else (i + 1) % count) for i in range(count)]
    return b, [(i, i ^ 1) for i in range(count)]


def local(
    pressure_now, pressure_before, class_map, courant_sq, source_cells, source_wavelet, layer_start
):
    shots, columns, depth, width = pressure_now.shape
    x_b, x_a = pairs(lax.axis_size("gx"))
    z_b, z_a = pairs(lax.axis_size("depth"))
    state = pltpu.VMEM((shots, columns + 2 * HALO, depth + 2 * ZO, width), F32)
    plane = pltpu.VMEM((columns, depth, width), F32)
    row = pltpu.VMEM((depth, width), F32)
    x_face = pltpu.VMEM((shots, HALO, depth, width), F32)
    z_face = pltpu.VMEM((shots, columns, HALO, width), F32)
    dense = jax.ShapeDtypeStruct((shots, columns, depth, width), F32)
    dma = pltpu.SemaphoreType.DMA
    tile = pltpu.VMEM((shots, columns, 8, width), F32)
    now = pltpu.with_memory_space_constraint(pressure_now, pltpu.HBM)
    before = pltpu.with_memory_space_constraint(pressure_before, pltpu.HBM)
    classes = pltpu.with_memory_space_constraint(class_map, pltpu.HBM)

    def swaps(send_b, send_a, send_near, send_far):
        got = []
        for array, axis, perm in (
            (send_b, "gx", x_b), (send_a, "gx", x_a), (send_near, "depth", z_b), (send_far, "depth", z_a)
        ):
            got.append(lax.ppermute(array, axis, perm))
        return got

    sends = call(open_kernel, [x_face, x_face, z_face, z_face], (now,), [ANY], scratch=[tile, tile, dma((4,))])
    got_b, got_a, got_near, got_far = swaps(*sends)
    u, v, w, sa, bc, spot, amp = call(
        begin_kernel,
        [state, state, plane, plane, row, pltpu.VMEM((8, width), jnp.int32), pltpu.VMEM((ITERS * shots, width), F32)],
        (courant_sq, layer_start, source_cells, source_wavelet, now, before, classes),
        [SMEM] * 4 + [ANY] * 3,
        scratch=[pltpu.VMEM((columns, depth, width), jnp.int32), dma((2 * shots + 1,))],
    )
    v = middle(0, spot, amp, u, v, w, sa, bc, state)
    for step in range(ITERS - 1):
        u, v = call(
            lambda *refs, step=step: ends_kernel(step, *refs),
            [state, state],
            (spot, amp, u, v, got_near, got_far, w, sa, bc),
            [VMEM] * 9,
            {2: 0, 3: 1},
        )
        u, v, send_near, send_far, send_b, send_a = call(
            lambda *refs, step=step: edge_kernel(step, *refs),
            [state, state, z_face, z_face, x_face, x_face],
            (spot, amp, u, v, got_b, got_a, w, sa, bc),
            [VMEM] * 9,
            {2: 0, 3: 1},
        )
        got_b, got_a, got_near, got_far = swaps(send_b, send_a, send_near, send_far)
        u, v = v, u
        v = middle(step + 1, spot, amp, u, v, w, sa, bc, state)
    (prior,) = call(prior_kernel, [dense], (u,), [VMEM], scratch=[dma((shots,))], out_specs=[ANY])
    last = ITERS - 1
    u, v, final = call(
        lambda *refs: ends_kernel(last, *refs),
        [state, state, dense],
        (spot, amp, u, v, got_near, got_far, w, sa, bc),
        [VMEM] * 9,
        {2: 0, 3: 1},
        scratch=[dma((shots,))],
        out_specs=[VMEM, VMEM, ANY],
    )
    _, _, final = call(
        lambda *refs: last_kernel(last, *refs),
        [state, state, dense],
        (spot, amp, u, v, final, got_b, got_a, w, sa, bc),
        [VMEM] * 4 + [ANY] + [VMEM] * 5,
        {2: 0, 3: 1, 4: 2},
        scratch=[dma((2 * shots,))],
        out_specs=[VMEM, VMEM, ANY],
    )
    return final, prior


def middle(step, spot, amp, u, v, w, sa, bc, state):
    return call(lambda *refs: middle_kernel(step, *refs), [state], (spot, amp, u, v, w, sa, bc), [VMEM] * 7, {3: 0})[0]


def solution(mesh):
    placed = (
        P(None, "gx", "depth", None),
        P(None, "gx", "depth", None),
        P("gx", "depth", None),
        P(),
        P(),
        P(),
        P(),
    )
    return jax.shard_map(
        local,
        mesh=mesh,
        in_specs=placed,
        out_specs=(P(None, "gx", "depth", None), P(None, "gx", "depth", None)),
        check_vma=False,
    )
```

```python
import jax
import jax.numpy as jnp
import numpy as np
from jax import lax
from jax.experimental import pallas as pl
from jax.experimental.pallas import tpu as pltpu
from jax.sharding import PartitionSpec as P


ITERS = 8
COEFFS = (-205.0 / 72.0, 8.0 / 5.0, -1.0 / 5.0, 8.0 / 315.0, -1.0 / 560.0)
DAMPING = 0.3
HALO = 4
ZO = 8
F32 = jnp.float32


def lanes(rows, width):
    return lax.broadcasted_iota(jnp.int32, (rows, width), 1)


def stencil(u, v, y, w, sa, bc, s, x, z, count):
    at = ZO + z
    center = u[s, HALO + x, at : at + count, :]
    total = None
    for k in range(1, HALO + 1):
        pair = u[s, HALO + x + k, at : at + count, :] + u[s, HALO + x - k, at : at + count, :]
        pair = pair + (u[s, HALO + x, at + k : at + k + count, :] + u[s, HALO + x, at - k : at - k + count, :])
        if k == 1:
            pair = pair + y[s, x, z : z + count, :]
        total = COEFFS[k] * pair if total is None else total + COEFFS[k] * pair
    return (
        w[x, z : z + count, :] * center
        + sa[x, z : z + count, :] * total
        - bc[z : z + count, :] * v[s, HALO + x, at : at + count, :]
    )


def halves(number):
    kind = np.dtype(jnp.bfloat16)
    high = float(np.asarray(number).astype(kind))
    return high, float(np.asarray(number - high).astype(kind))


def fill_band(band):
    size = band.shape[0]
    width = size // 2
    i = lax.broadcasted_iota(jnp.int32, (size, size), 0)
    j = lax.broadcasted_iota(jnp.int32, (size, size), 1)
    right, below = j >= width, i >= width
    apart = jnp.abs(jnp.where(below, i - width, i) - jnp.where(right, j - width, j))
    high, low = jnp.zeros((size, size), F32), jnp.zeros((size, size), F32)
    for k in range(1, HALO + 1):
        parts = halves(COEFFS[k] / COEFFS[1])
        high = jnp.where(apart == k, parts[0], high)
        low = jnp.where(apart == k, parts[1], low)
    band[...] = jnp.where(right, jnp.where(below, 0.0, low), high).astype(jnp.bfloat16)


def lateral(u, band, y):
    shots, columns, depth, width = y.shape

    def shot(s, carry):
        now = u[s, HALO : HALO + columns, ZO : ZO + depth, :].reshape(columns * depth, width)
        high = now.astype(jnp.bfloat16)
        low = (now - high.astype(F32)).astype(jnp.bfloat16)
        both = jnp.dot(jnp.concatenate([high, low], axis=1), band[...], preferred_element_type=F32)
        y[s] = (both[:, :width] + both[:, width:]).reshape(columns, depth, width)
        return carry

    lax.fori_loop(0, shots, shot, 0)


def inject(step, spot, amp, v, spans, send=None, send_at=None):
    shots, width = v.shape[0], v.shape[3]
    depth = v.shape[2] - 2 * ZO

    @pl.when(spot[shots : shots + 1, :][0, 0] >= 0)
    def _():
        for s in range(shots):
            flat = spot[s : s + 1, :][0, 0]
            x = lax.div(flat, depth * width)
            z = lax.rem(lax.div(flat, width), depth)
            y = lax.rem(flat, width)
            for x_low, x_high, z_low, z_high in spans:

                @pl.when((flat >= 0) & (x >= x_low) & (x < x_high) & (z >= z_low) & (z < z_high))
                def _():
                    at = step * shots + s
                    add = jnp.where(lanes(1, width) == y, amp[at : at + 1, :], 0.0)
                    row = v[s, HALO + x, pl.ds(ZO + z, 1), :] + add
                    v[s, HALO + x, pl.ds(ZO + z, 1), :] = row
                    if send is not None:
                        send[s, x - send_at, pl.ds(z, 1), :] = row


def at_high_x(side):
    odd = lax.rem(lax.axis_index("gx"), 2)
    return odd if side == 0 else 1 - odd


def at_end(axis):
    place = lax.axis_index(axis)
    return (place == 0) | (place == lax.axis_size(axis) - 1)


def fill_depth(u, z_near, z_far, columns, depth):
    odd = lax.rem(lax.axis_index("depth"), 2) == 1
    inside = jnp.where(at_end("depth"), 0.0, 1.0).astype(F32)

    def some(x, carry):
        for s in range(u.shape[0]):
            far = z_far[s, x]
            near = z_near[s, x] * inside
            u[s, HALO + x, ZO - HALO : ZO, :] = jnp.where(odd, far, near)
            u[s, HALO + x, ZO + depth : ZO + depth + HALO, :] = jnp.where(odd, near, far)
        return carry

    lax.fori_loop(0, columns, some, 0, unroll=8)


def fill_x(side, u, got, columns, depth):
    at = at_high_x(side) * (columns + HALO)
    inside = jnp.where(at_end("gx"), 0.0, 1.0).astype(F32)
    for s in range(u.shape[0]):
        for x in range(HALO):
            row = got[s, x]
            u[s, at + x, ZO : ZO + depth, :] = row * inside if side == 0 else row


def depth_faces(v, send_near, send_far, columns, depth):
    odd = lax.rem(lax.axis_index("depth"), 2) == 1

    def face(x, carry):
        for s in range(v.shape[0]):
            low = v[s, HALO + x, ZO : ZO + HALO, :]
            high = v[s, HALO + x, ZO + depth - HALO : ZO + depth, :]
            send_near[s, x] = jnp.where(odd, high, low)
            send_far[s, x] = jnp.where(odd, low, high)
        return carry

    lax.fori_loop(0, columns, face, 0, unroll=8)


def span_loop(u, v, y, w, sa, bc, tiles, group):
    inner = w.shape[0] - 2 * HALO

    def some(i, carry):
        s, x = i // (inner // group), HALO + group * lax.rem(i, inner // group)
        for j in range(group):
            for z, count in tiles:
                v[s, HALO + x + j, ZO + z : ZO + z + count, :] = stencil(u, v, y, w, sa, bc, s, x + j, z, count)
        return carry

    lax.fori_loop(0, v.shape[0] * (inner // group), some, 0)


def ends_kernel(step, spot, amp, u_in, v_in, z_near, z_far, y, w, sa, bc, u, v, *out):
    del u_in, v_in
    columns, depth = w.shape[0], w.shape[1]
    fill_depth(u, z_near, z_far, columns, depth)
    span_loop(u, v, y, w, sa, bc, ((0, 8), (depth - 8, 8)), 12)
    inject(step, spot, amp, v, ((HALO, columns - HALO, 0, 8), (HALO, columns - HALO, depth - 8, depth)))
    if step == ITERS - 1:
        to_hbm(v, *out, ((HALO, columns - 2 * HALO),))


def middle_kernel(step, spot, amp, u, v_in, band, w, sa, bc, v, y):
    del v_in
    lateral(u, band, y)
    columns, depth = w.shape[0], w.shape[1]
    span_loop(u, v, y, w, sa, bc, ((8, depth - 16),), 12)
    inject(step, spot, amp, v, ((HALO, columns - HALO, 8, depth - 8),))


def edge_kernel(step, spot, amp, u_in, v_in, got_b, got_a, y, w, sa, bc, u, v, near, far, send_b, send_a):
    del u_in, v_in
    columns, depth = w.shape[0], w.shape[1]
    fill_x(0, u, got_b, columns, depth)
    fill_x(1, u, got_a, columns, depth)
    for s in range(u.shape[0]):
        for x in range(HALO):
            for side, send in ((0, send_b), (1, send_a)):
                at = at_high_x(side) * (columns - HALO) + x
                new = stencil(u, v, y, w, sa, bc, s, at, 0, depth)
                v[s, HALO + at, ZO : ZO + depth, :] = new
                send[s, x] = new
    for side, send in ((0, send_b), (1, send_a)):
        face = at_high_x(side) * (columns - HALO)
        inject(step, spot, amp, v, ((face, face + HALO, 0, depth),), send, face)
    depth_faces(v, near, far, columns, depth)


def last_kernel(step, spot, amp, u_in, v_in, out_in, got_b, got_a, y, w, sa, bc, u, v, out, sem):
    del u_in, v_in, out_in
    columns, depth = w.shape[0], w.shape[1]
    fill_x(0, u, got_b, columns, depth)
    fill_x(1, u, got_a, columns, depth)
    for s in range(u.shape[0]):
        for x in range(HALO):
            for at in (x, columns - HALO + x):
                v[s, HALO + at, ZO : ZO + depth, :] = stencil(u, v, y, w, sa, bc, s, at, 0, depth)
    inject(step, spot, amp, v, ((0, HALO, 0, depth), (columns - HALO, columns, 0, depth)))
    to_hbm(v, out, sem, ((0, HALO), (columns - HALO, HALO)))


def to_hbm(v, out, sem, spans):
    shots, depth = out.shape[0], out.shape[2]
    copies = []
    for i, (first, count) in enumerate(spans):
        for s in range(shots):
            source = v.at[s, pl.ds(HALO + first, count), pl.ds(ZO, depth), :]
            copies.append(pltpu.make_async_copy(source, out.at[s, pl.ds(first, count)], sem.at[i * shots + s]))
    for c in copies:
        c.start()
    for c in copies:
        c.wait()


def prior_kernel(u, out, sem):
    to_hbm(u, out, sem, ((0, out.shape[1]),))


def open_kernel(now, send_b, send_a, send_near, send_far, low, high, sem):
    shots, columns, depth = now.shape[0], now.shape[1], now.shape[2]
    copies = []
    for target, source in (
        (low, now.at[:, :, pl.ds(0, 8)]),
        (high, now.at[:, :, pl.ds(depth - 8, 8)]),
        (send_b, now.at[:, pl.ds(at_high_x(0) * (columns - HALO), HALO)]),
        (send_a, now.at[:, pl.ds(at_high_x(1) * (columns - HALO), HALO)]),
    ):
        copies.append(pltpu.make_async_copy(source, target, sem.at[len(copies)]))
    for c in copies:
        c.start()
    odd = lax.rem(lax.axis_index("depth"), 2) == 1
    copies[0].wait()
    copies[1].wait()

    def face(x, carry):
        for s in range(shots):
            first, last = low[s, x, 0:HALO, :], high[s, x, 8 - HALO : 8, :]
            send_near[s, x] = jnp.where(odd, last, first)
            send_far[s, x] = jnp.where(odd, first, last)
        return carry

    lax.fori_loop(0, columns, face, 0, unroll=8)
    copies[2].wait()
    copies[3].wait()


def begin_kernel(speeds, start, cells, wavelet, now, before, classes, u, v, w, sa, bc, spot, amp, band, kinds, sem):
    shots, columns, depth, width = now.shape
    copies = [pltpu.make_async_copy(classes, kinds, sem.at[2 * shots])]
    for i, (source, state) in enumerate(((now, u), (before, v))):
        for s in range(shots):
            target = state.at[s, pl.ds(HALO, columns), pl.ds(ZO, depth), :]
            copies.append(pltpu.make_async_copy(source.at[s], target, sem.at[i * shots + s]))
    for c in copies:
        c.start()
    total = depth * lax.axis_size("depth")
    first_x, first_z = lax.axis_index("gx") * columns, lax.axis_index("depth") * depth
    begin = start[0]

    def damping_at(z):
        ratio = (z - begin + 1).astype(F32) / jnp.broadcast_to((total - begin).astype(F32), z.shape)
        return jnp.where(z >= begin, DAMPING * ratio * ratio, 0.0)

    damping = damping_at(first_z + lax.broadcasted_iota(jnp.int32, (depth, width), 0))
    inverse = 1.0 / (1.0 + damping)
    bc[...] = (1.0 - damping) * inverse
    some = jnp.int32(-1)
    for s in range(shots):
        x, z, y = cells[s, 0] - first_x, cells[s, 1] - first_z, cells[s, 2]
        mine = (x >= 0) & (x < columns) & (z >= 0) & (z < depth)
        flat = jnp.where(mine, (x * depth + z) * width + y, -1)
        some = jnp.maximum(some, flat)
        spot[s : s + 1, :] = jnp.broadcast_to(flat, (1, width))
        scale = 1.0 / (1.0 + damping_at(jnp.broadcast_to(cells[s, 1], (1, width))))
        for step in range(wavelet.shape[0]):
            amp[step * shots + s : step * shots + s + 1, :] = wavelet[step, s] * scale
    spot[shots : shots + 1, :] = jnp.broadcast_to(some, (1, width))
    fill_band(band)
    copies[0].wait()

    def column(x, carry):
        kind = kinds[x]
        speed = jnp.zeros((depth, width), F32)
        for c in range(speeds.shape[0]):
            speed = jnp.where(kind == c, speeds[c], speed)
        scaled = speed * inverse
        sa[x] = scaled
        w[x] = 2.0 * inverse + (3.0 * COEFFS[0]) * scaled
        return carry

    lax.fori_loop(0, columns, column, 0, unroll=2)
    for c in copies[1:]:
        c.wait()


VMEM = pl.BlockSpec(memory_space=pltpu.VMEM)
SMEM = pl.BlockSpec(memory_space=pltpu.SMEM)
ANY = pl.BlockSpec(memory_space=pl.ANY)


def call(kernel, out_shape, args, specs, aliases=None, flops=1_000_000, scratch=(), out_specs=None):
    return pl.pallas_call(
        kernel,
        out_shape=out_shape,
        in_specs=specs,
        out_specs=out_specs if out_specs is not None else [VMEM] * len(out_shape),
        input_output_aliases=aliases or {},
        scratch_shapes=list(scratch),
        cost_estimate=pl.CostEstimate(flops=flops, bytes_accessed=4_000_000, transcendentals=0),
        compiler_params=pltpu.CompilerParams(vmem_limit_bytes=16 * 1024 * 1024),
    )(*args)


def pairs(count):
    b = [(i, (i - 1) % count if i % 2 == 0 else (i + 1) % count) for i in range(count)]
    return b, [(i, i ^ 1) for i in range(count)]


def local(
    pressure_now, pressure_before, class_map, courant_sq, source_cells, source_wavelet, layer_start
):
    shots, columns, depth, width = pressure_now.shape
    x_b, x_a = pairs(lax.axis_size("gx"))
    z_b, z_a = pairs(lax.axis_size("depth"))
    state = pltpu.VMEM((shots, columns + 2 * HALO, depth + 2 * ZO, width), F32)
    lateral_sums = pltpu.VMEM((shots, columns, depth, width), F32)
    plane = pltpu.VMEM((columns, depth, width), F32)
    row = pltpu.VMEM((depth, width), F32)
    x_face = pltpu.VMEM((shots, HALO, depth, width), F32)
    z_face = pltpu.VMEM((shots, columns, HALO, width), F32)
    dense = jax.ShapeDtypeStruct((shots, columns, depth, width), F32)
    dma = pltpu.SemaphoreType.DMA
    tile = pltpu.VMEM((shots, columns, 8, width), F32)
    now = pltpu.with_memory_space_constraint(pressure_now, pltpu.HBM)
    before = pltpu.with_memory_space_constraint(pressure_before, pltpu.HBM)
    classes = pltpu.with_memory_space_constraint(class_map, pltpu.HBM)

    def swaps(send_b, send_a, send_near, send_far):
        got = []
        for array, axis, perm in (
            (send_b, "gx", x_b), (send_a, "gx", x_a), (send_near, "depth", z_b), (send_far, "depth", z_a)
        ):
            got.append(lax.ppermute(array, axis, perm))
        return got

    sends = call(open_kernel, [x_face, x_face, z_face, z_face], (now,), [ANY], scratch=[tile, tile, dma((4,))])
    got_b, got_a, got_near, got_far = swaps(*sends)
    u, v, w, sa, bc, spot, amp, band = call(
        begin_kernel,
        [
            state,
            state,
            plane,
            plane,
            row,
            pltpu.VMEM((8, width), jnp.int32),
            pltpu.VMEM((ITERS * shots, width), F32),
            pltpu.VMEM((2 * width, 2 * width), jnp.bfloat16),
        ],
        (courant_sq, layer_start, source_cells, source_wavelet, now, before, classes),
        [SMEM] * 4 + [ANY] * 3,
        scratch=[pltpu.VMEM((columns, depth, width), jnp.int32), dma((2 * shots + 1,))],
    )
    v, y = middle(0, spot, amp, u, v, band, w, sa, bc, state, lateral_sums)
    for step in range(ITERS - 1):
        u, v = call(
            lambda *refs, step=step: ends_kernel(step, *refs),
            [state, state],
            (spot, amp, u, v, got_near, got_far, y, w, sa, bc),
            [VMEM] * 10,
            {2: 0, 3: 1},
        )
        u, v, send_near, send_far, send_b, send_a = call(
            lambda *refs, step=step: edge_kernel(step, *refs),
            [state, state, z_face, z_face, x_face, x_face],
            (spot, amp, u, v, got_b, got_a, y, w, sa, bc),
            [VMEM] * 10,
            {2: 0, 3: 1},
        )
        got_b, got_a, got_near, got_far = swaps(send_b, send_a, send_near, send_far)
        u, v = v, u
        v, y = middle(step + 1, spot, amp, u, v, band, w, sa, bc, state, lateral_sums)
    (prior,) = call(prior_kernel, [dense], (u,), [VMEM], scratch=[dma((shots,))], out_specs=[ANY])
    last = ITERS - 1
    u, v, final = call(
        lambda *refs: ends_kernel(last, *refs),
        [state, state, dense],
        (spot, amp, u, v, got_near, got_far, y, w, sa, bc),
        [VMEM] * 10,
        {2: 0, 3: 1},
        scratch=[dma((shots,))],
        out_specs=[VMEM, VMEM, ANY],
    )
    _, _, final = call(
        lambda *refs: last_kernel(last, *refs),
        [state, state, dense],
        (spot, amp, u, v, final, got_b, got_a, y, w, sa, bc),
        [VMEM] * 4 + [ANY] + [VMEM] * 6,
        {2: 0, 3: 1, 4: 2},
        scratch=[dma((2 * shots,))],
        out_specs=[VMEM, VMEM, ANY],
    )
    return final, prior


def middle(step, spot, amp, u, v, band, w, sa, bc, state, lateral_sums):
    return call(
        lambda *refs: middle_kernel(step, *refs),
        [state, lateral_sums],
        (spot, amp, u, v, band, w, sa, bc),
        [VMEM] * 8,
        {3: 0},
    )


def solution(mesh):
    placed = (
        P(None, "gx", "depth", None),
        P(None, "gx", "depth", None),
        P("gx", "depth", None),
        P(),
        P(),
        P(),
        P(),
    )
    return jax.shard_map(
        local,
        mesh=mesh,
        in_specs=placed,
        out_specs=(P(None, "gx", "depth", None), P(None, "gx", "depth", None)),
        check_vma=False,
    )
```
